32 devices in a mesh: gx: 4 (over y, x), gy: 8 (over z, core).
Axes of the slice: x: 2, y: 2, z: 4, core: 2. Of those that a mesh axis runs over, the one named last changes fastest.
Arguments:
- right_side: float32 [128, 2048], P('gx', 'gy'), may hold values from -200 to 200
- reaction: float32 [128, 2048], P('gx', 'gy'), may hold values from 2 to 4
- kernel: float32 [65, 65], replicated, may hold values from -0.04 to 0.04
Outputs:
- solution: float32 [128, 2048], P('gx', 'gy')
- residual: float32 [128, 2048], P('gx', 'gy')
The draws below stay inside these ranges and needn't reach their ends.
All inputs are finite; a program needn't handle non-finite values.
Results may differ from the reference program's by a relative error of at most 0.00075.
Values sent between devices are 32-bit elements; how exact they have to be, the bound alone decides.
A program may use at most 64 MiB of HBM per device.

```python
import jax
import jax.numpy as jnp
from jax import lax

RAD = 32
ITERS = 4
NX = 128
NY = 2048


def draw_right_side(key, part):
    key_base, key_rows, key_cols = jax.random.split(jax.random.fold_in(key, 17), 3)
    row_pos = jnp.arange(NX, dtype=jnp.float32) / NX
    col_pos = jnp.arange(NY, dtype=jnp.float32) / NY
    row_rough = jax.random.uniform(key_rows, (NX,), jnp.float32)
    col_rough = jax.random.uniform(key_cols, (NY,), jnp.float32)
    base = jnp.clip(jax.random.normal(key_base, (NX, NY), jnp.float32), -5.0, 5.0)
    trend = 3.0
    scale = trend ** (row_pos[:, None] + col_pos[None, :]) * 10.0 ** (0.5 * (row_rough[:, None] + col_rough[None, :])) / 10.0
    return base * scale


def level_of(stream_key, shape, cuts, smallest, high):
    def one(dim, shards_of):
        heights = jax.random.uniform(jax.random.fold_in(jax.random.fold_in(stream_key, 6), dim), (shards_of,), jnp.float32, smallest / len(cuts), high / len(cuts))
        return jnp.repeat(jnp.exp(heights), shape[dim] // shards_of).reshape((-1,) + (1,) * (len(shape) - dim - 1))

    level = one(*cuts[0])
    for cut in cuts[1:]:
        level = level * one(*cut)
    return level


def noise(stream_key, shape, deviation, limit, held_as=jnp.bfloat16):
    array = jax.random.normal(stream_key, shape, jnp.float32) * deviation
    return jnp.minimum(jnp.maximum(array, -limit), limit).astype(held_as)


def setup_inputs(seed: int = 0) -> dict:
    splits = jax.random.split(jax.random.key(seed), 4)
    right_side = draw_right_side(jax.random.fold_in(splits[3], 71), 0)
    reaction = jnp.clip(2.0 + 2.0 * jax.random.uniform(splits[1], (NX, NY), jnp.float32) ** level_of(splits[1], (NX, NY), ((0, 4), (1, 8)), -0.2, 0.2), 2.0, 4.0)
    kernel = noise(splits[2], (2 * RAD + 1, 2 * RAD + 1), 0.0077, 0.04, jnp.float32)
    return dict(right_side=right_side, reaction=reaction, kernel=kernel)


small_term = 1e-06

def apply_operator(values, reaction, kernel):
    total_rows = NX + 2 * RAD
    total_cols = NY + 2 * RAD
    spectrum = jnp.fft.rfft2(values, s=(total_rows, total_cols)) * jnp.fft.rfft2(kernel, s=(total_rows, total_cols))
    linear = jnp.fft.irfft2(spectrum, s=(total_rows, total_cols))
    return reaction * values - linear[RAD:RAD + NX, RAD:RAD + NY]

def solve_small(normal_matrix, target):
    factor = jnp.linalg.cholesky(normal_matrix)
    forward = []
    for position in range(ITERS):
        accum = target[position]
        for earlier in range(position):
            accum = accum - factor[position, earlier] * forward[earlier]
        forward.append(accum / factor[position, position])
    backward = [None] * ITERS
    for position in reversed(range(ITERS)):
        accum = forward[position]
        for later in range(position + 1, ITERS):
            accum = accum - factor[later, position] * backward[later]
        backward[position] = accum / factor[position, position]
    return backward

def reference(right_side, reaction, kernel):
    initial_norm = jnp.sqrt(jnp.sum(right_side * right_side) + small_term)
    krylov = [right_side / initial_norm]
    upper = jnp.zeros((ITERS + 1, ITERS), jnp.float32)
    for column in range(ITERS):
        candidate = apply_operator(krylov[column], reaction, kernel)
        for earlier in range(column + 1):
            projected = jnp.sum(candidate * krylov[earlier])
            candidate = candidate - projected * krylov[earlier]
            upper = upper.at[earlier, column].set(projected)
        length = jnp.sqrt(jnp.sum(candidate * candidate) + small_term)
        upper = upper.at[column + 1, column].set(length)
        krylov.append(candidate / length)
    normal_matrix = jnp.dot(upper.T, upper, precision=lax.Precision.HIGHEST)
    coeffs = solve_small(normal_matrix, initial_norm * upper[0, :])
    solution = coeffs[0] * krylov[0]
    for column in range(1, ITERS):
        solution = solution + coeffs[column] * krylov[column]
    residual = right_side - apply_operator(solution, reaction, kernel)
    return (solution, residual)
```

```python
import functools

import jax
import jax.numpy as jnp
from jax import lax
from jax.experimental import pallas as pl
from jax.experimental.pallas import tpu as pltpu
from jax.sharding import PartitionSpec as P

ITERS = 4
SHIFT = 3.0
SMALL = 1e-06
LANES = 128
FOLD = 8
MESH = pl.DeviceIdType.MESH
F32 = jnp.float32
BF16 = jnp.bfloat16


def split(values):
    high = values.astype(BF16)
    return high, (values - high.astype(F32)).astype(BF16)


def lane_group(shape, width):
    return lax.broadcasted_iota(jnp.int32, shape, 1) // width


def pick(group, parts):
    chosen = parts[0]
    for index in range(1, len(parts)):
        chosen = jnp.where(group == index, parts[index], chosen)
    return chosen


def solve(gram):
    count = ITERS + 1
    initial = jnp.sqrt(gram[0][0] + SMALL)
    basis = [[1.0 / initial]]
    images = []
    applied = []
    upper = [[None] * ITERS for _ in range(count)]

    def times_gram(vector):
        out = []
        for row in range(count):
            total = vector[0] * gram[row][0]
            for col in range(1, len(vector)):
                total = total + vector[col] * gram[row][col]
            out.append(total)
        return out

    def inner(left, right):
        total = left[0] * right[0]
        for index in range(1, len(left)):
            total = total + left[index] * right[index]
        return total

    images.append(times_gram(basis[0]))
    for column in range(ITERS):
        prior = basis[column]
        candidate = [SHIFT * prior[0]]
        for index in range(1, len(prior)):
            candidate.append(SHIFT * prior[index] + prior[index - 1])
        candidate.append(prior[-1])
        applied.append(list(candidate))
        for earlier in range(column + 1):
            projected = inner(candidate, images[earlier])
            for index, value in enumerate(basis[earlier]):
                candidate[index] = candidate[index] - projected * value
            upper[earlier][column] = projected
        square = jnp.maximum(inner(candidate, times_gram(candidate)), 0.0)
        length = jnp.sqrt(square + SMALL)
        upper[column + 1][column] = length
        if column + 1 < ITERS:
            inverse = 1.0 / length
            basis.append([value * inverse for value in candidate])
            images.append(times_gram(basis[-1]))

    normal = [[None] * ITERS for _ in range(ITERS)]
    for row in range(ITERS):
        for col in range(row + 1):
            total = None
            for index in range(col + 2):
                term = upper[index][row] * upper[index][col]
                total = term if total is None else total + term
            normal[row][col] = total
    factor = [[None] * ITERS for _ in range(ITERS)]
    inverse = [None] * ITERS
    for col in range(ITERS):
        for row in range(col, ITERS):
            accum = normal[row][col]
            for index in range(col):
                accum = accum - factor[row][index] * factor[col][index]
            if row == col:
                factor[row][col] = jnp.sqrt(accum)
                inverse[col] = 1.0 / factor[row][col]
            else:
                factor[row][col] = accum * inverse[col]
    forward = []
    for row in range(ITERS):
        accum = initial * upper[0][row]
        for index in range(row):
            accum = accum - factor[row][index] * forward[index]
        forward.append(accum * inverse[row])
    coeffs = [None] * ITERS
    for row in reversed(range(ITERS)):
        accum = forward[row]
        for index in range(row + 1, ITERS):
            accum = accum - factor[index][row] * coeffs[index]
        coeffs[row] = accum * inverse[row]

    def combine(vectors, size):
        out = []
        for index in range(size):
            total = None
            for coeff, vector in zip(coeffs, vectors):
                if index < len(vector):
                    term = coeff * vector[index]
                    total = term if total is None else total + term
            out.append(total)
        return out

    return combine(basis, ITERS), combine(applied, count)


def kernel(
    nx, ny, b_ref, reac_ref, k_ref, x_ref, r_ref,
    kpad, whi, wlo, ybuf, wbuf, ebuf, hrow, hedge, gall, gown,
    row_send, row_recv, edge_send, edge_recv, g_send, g_recv,
):
    rows, cols = b_ref.shape
    width = k_ref.shape[0]
    rad = width // 2
    span = rows + 2 * rad
    tiles = cols // LANES
    subs = rows // 8
    count = nx * ny
    gx, gy = lax.axis_index("gx"), lax.axis_index("gy")
    me = gx * ny + gy

    hrow[...] = jnp.zeros_like(hrow)
    hedge[...] = jnp.zeros_like(hedge)

    barrier = pltpu.get_barrier_semaphore()

    def other(step):
        target = lax.rem(me + step, count)
        return (target // ny, lax.rem(target, ny))

    def greet(step, carry):
        pl.semaphore_signal(barrier, inc=1, device_id=other(step), device_id_type=MESH)
        return carry

    lax.fori_loop(1, count, greet, 0)

    exists_x = {-1: gx > 0, 0: None, 1: gx < nx - 1}
    exists_y = {-1: gy > 0, 1: gy < ny - 1}

    def both(dx, dy):
        if dx == 0:
            return exists_y[dy]
        if dy == 0:
            return exists_x[dx]
        return jnp.logical_and(exists_x[dx], exists_y[dy])

    def source(step):
        return b_ref if step == 0 else wbuf.at[step - 1]

    def row_copy(step, dx):
        slot = 0 if dx == 1 else 1
        return pltpu.make_async_remote_copy(
            src_ref=source(step), dst_ref=hrow.at[step, slot],
            send_sem=row_send.at[step, slot], recv_sem=row_recv.at[step, slot],
            device_id=(gx + dx, gy), device_id_type=MESH,
        )

    def edge_copy(step, dx, dy):
        side = 1 if dy == -1 else 0
        group = 1 - dx
        return pltpu.make_async_remote_copy(
            src_ref=ebuf.at[step, side], dst_ref=hedge.at[step, side, group],
            send_sem=edge_send.at[step, side, group], recv_sem=edge_recv.at[step, side, group],
            device_id=(gx + dx, gy + dy), device_id_type=MESH,
        )

    edges = [(dx, dy) for dx in (-1, 1, 0) for dy in (-1, 1)]

    def start_all(step):
        for dx in (-1, 1):
            pl.when(both(dx, 0))(lambda dx=dx: row_copy(step, dx).start())
        for dx, dy in edges:
            pl.when(both(dx, dy))(lambda dx=dx, dy=dy: edge_copy(step, dx, dy).start())

    def wait_recv_all(step):
        for dx in (-1, 1):
            pl.when(both(-dx, 0))(lambda dx=dx: row_copy(step, dx).wait_recv())
        for dx, dy in edges:
            pl.when(both(-dx, -dy))(lambda dx=dx, dy=dy: edge_copy(step, dx, dy).wait_recv())

    def wait_send_all(step):
        for dx in (-1, 1):
            pl.when(both(dx, 0))(lambda dx=dx: row_copy(step, dx).wait_send())
        for dx, dy in edges:
            pl.when(both(dx, dy))(lambda dx=dx, dy=dy: edge_copy(step, dx, dy).wait_send())

    group8 = lane_group((8, LANES), rad)

    def pack_edges(step, values):
        first = values[:, :LANES]
        last = values[:, cols - LANES:]
        lefts, rights = [], []
        for t in range(subs):
            piece = first[8 * t: 8 * t + 8]
            lefts.append(pltpu.roll(piece, (rad * t) % LANES, 1) if t else piece)
            piece = last[8 * t: 8 * t + 8]
            move = (rad * t - (LANES - rad)) % LANES
            rights.append(pltpu.roll(piece, move, 1) if move else piece)
        ebuf[step, 1] = pick(group8, lefts)
        ebuf[step, 0] = pick(group8, rights)

    pack_edges(0, b_ref[...])

    kpad[...] = jnp.zeros_like(kpad)
    kpad[:width, :width] = k_ref[...]
    kpad[...] = kpad[...].T
    group_span = lane_group((span, LANES), rows)
    per_tile = LANES // rows
    blocks = -(-width // (2 * FOLD))
    whole = FOLD * rows
    for q in range(blocks):
        for h in range(2):
            first = 2 * FOLD * q + FOLD * h
            base = (2 * q + h) * LANES
            for t in range(whole // LANES):
                parts = []
                for u in range(per_tile):
                    b = first + per_tile * t + u
                    if b < width:
                        line = jnp.broadcast_to(kpad[b: b + 1, :], (span, LANES))
                        move = (rows * u - 2 * rad) % LANES
                        parts.append(pltpu.roll(line, move, 1, stride=1, stride_axis=0))
                    else:
                        parts.append(jnp.zeros((span, LANES), F32))
                block = pick(group_span, parts)
                block = jnp.concatenate([block, jnp.zeros((LANES - span, LANES), F32)], axis=0)
                high, low = split(block)
                whi[base: base + LANES, t * LANES: (t + 1) * LANES] = high
                wlo[base: base + LANES, t * LANES: (t + 1) * LANES] = low

    pl.semaphore_wait(barrier, count - 1)
    start_all(0)

    steps_m = cols + 2 * FOLD
    group_cols = lane_group((cols, LANES), rows)
    offset = reac_ref[...] - SHIFT

    def fold8(values):
        total = values[:8]
        for t in range(1, subs):
            total = total + values[8 * t: 8 * t + 8]
        out = total[:, :LANES]
        for t in range(1, tiles):
            out = out + total[:, t * LANES: (t + 1) * LANES]
        return jnp.sum(out, axis=0, keepdims=True)

    vectors = [b_ref[...]]
    products = {(0, 0): fold8(vectors[0] * vectors[0])}

    for step in range(ITERS):
        own = vectors[step]
        wait_recv_all(step)
        above, below = hrow[step, 0], hrow[step, 1]
        blank = jnp.zeros((LANES - span, LANES), F32)
        centre = []
        for t in range(tiles):
            part = slice(t * LANES, (t + 1) * LANES)
            tile = jnp.concatenate([above[:, part], own[:, part], below[:, part], blank], axis=0)
            centre.append(tile.T)
        sides = []
        for group in range(3):
            left = hedge[step, 0, group]
            right = hedge[step, 1, group] if True else None
            for t in range(subs):
                move = (-rad * t) % LANES
                from_left = pltpu.roll(left, move, 1) if move else left
                move = (rad - rad * t) % LANES
                from_right = pltpu.roll(right, move, 1) if move else right
                sides.append(jnp.where(group8 == 0, from_left, from_right))
        side = jnp.concatenate(sides + [blank], axis=0).T
        padded = jnp.concatenate([side[:rad]] + centre + [side[rad: 2 * rad]], axis=0)
        zero = jnp.zeros((FOLD, LANES), F32)
        plain = jnp.concatenate([zero] * 3 + [padded] + [zero], axis=0)
        moved = jnp.concatenate([zero] * 4 + [padded], axis=0)
        high, low = split(jnp.concatenate([plain, moved], axis=1))
        top = 2 * FOLD * blocks
        take = lambda m: jnp.concatenate(
            [m[top - 2 * FOLD * q: top - 2 * FOLD * q + steps_m] for q in range(blocks)], axis=1
        )
        lhs_high, lhs_low = take(high), take(low)
        dot = functools.partial(jnp.dot, preferred_element_type=F32)
        ybuf[...] = dot(lhs_high, whi[...]) + dot(lhs_low, whi[...]) + dot(lhs_high, wlo[...])
        parts = []
        for u in range(per_tile):
            total = None
            for t in range(whole // LANES):
                start = FOLD - per_tile * t - u
                piece = ybuf[start: start + cols, t * LANES: (t + 1) * LANES]
                total = piece if total is None else total + piece
            parts.append(total)
        chosen = pick(group_cols, parts)
        pieces = []
        for t in range(tiles):
            turned = chosen[t * LANES: (t + 1) * LANES].T
            total = turned[:rows]
            for u in range(1, per_tile):
                total = total + turned[rows * u: rows * (u + 1)]
            pieces.append(total)
        fresh = offset * own - jnp.concatenate(pieces, axis=1)
        wbuf[step] = fresh
        if step + 1 < ITERS:
            pack_edges(step + 1, fresh)
            start_all(step + 1)
        vectors.append(fresh)
        for earlier in range(step + 2):
            products[(earlier, step + 1)] = fold8(vectors[earlier] * fresh)

    order = sorted(products)
    stack = [products[pair] for pair in order]
    table = jnp.concatenate(stack + [jnp.zeros((LANES - len(stack), LANES), F32)], axis=0)
    line = jnp.sum(table.T, axis=0, keepdims=True)
    gown[...] = line
    gall[me] = line

    def gram_copy(step):
        return pltpu.make_async_remote_copy(
            src_ref=gown, dst_ref=gall.at[me],
            send_sem=g_send.at[step], recv_sem=g_recv.at[me],
            device_id=other(step), device_id_type=MESH,
        )

    def gram_arrival(step):
        sender = lax.rem(me + step, count)
        return pltpu.make_async_remote_copy(
            src_ref=gown, dst_ref=gall.at[sender],
            send_sem=g_send.at[step], recv_sem=g_recv.at[sender],
            device_id=other(step), device_id_type=MESH,
        )

    def send(step, carry):
        gram_copy(step).start()
        return carry

    def receive(step, carry):
        gram_arrival(step).wait_recv()
        return carry

    def sent(step, carry):
        gram_copy(step).wait_send()
        return carry

    lax.fori_loop(1, count, send, 0)
    for step in range(ITERS):
        wait_send_all(step)
    lax.fori_loop(1, count, receive, 0)
    total = jnp.sum(gall[...], axis=0)
    spread = jnp.broadcast_to(total, (LANES, LANES)).T
    gram = [[None] * (ITERS + 1) for _ in range(ITERS + 1)]
    for index, (i, j) in enumerate(order):
        gram[i][j] = gram[j][i] = spread[index: index + 1]
    at_solution, at_applied = solve(gram)
    wide = lambda value: jnp.concatenate([value] * tiles, axis=1)
    answer = wide(at_solution[0]) * vectors[0]
    for index in range(1, ITERS):
        answer = answer + wide(at_solution[index]) * vectors[index]
    x_ref[...] = answer
    image = wide(at_applied[0]) * vectors[0]
    for index in range(1, ITERS + 1):
        image = image + wide(at_applied[index]) * vectors[index]
    r_ref[...] = vectors[0] - image
    lax.fori_loop(1, count, sent, 0)


def solution(mesh):
    nx, ny = mesh.shape["gx"], mesh.shape["gy"]
    count = nx * ny

    def local(right_side, reaction, weights):
        rows, cols = right_side.shape
        width = weights.shape[0]
        blocks = -(-width // (2 * FOLD))
        depth = blocks * 2 * LANES
        block = jax.ShapeDtypeStruct((rows, cols), F32)
        in_vmem = pl.BlockSpec(memory_space=pltpu.VMEM)
        dma = pltpu.SemaphoreType.DMA
        return pl.pallas_call(
            functools.partial(kernel, nx, ny),
            name="gmres_cycle",
            out_shape=(block, block),
            in_specs=[in_vmem] * 3,
            out_specs=(in_vmem, in_vmem),
            scratch_shapes=[
                pltpu.VMEM((LANES, LANES), F32),
                pltpu.VMEM((depth, FOLD * rows), BF16),
                pltpu.VMEM((depth, FOLD * rows), BF16),
                pltpu.VMEM((cols + 2 * FOLD, FOLD * rows), F32),
                pltpu.VMEM((ITERS, rows, cols), F32),
                pltpu.VMEM((ITERS, 2, 8, LANES), F32),
                pltpu.VMEM((ITERS, 2, rows, cols), F32),
                pltpu.VMEM((ITERS, 2, 3, 8, LANES), F32),
                pltpu.VMEM((count, 1, LANES), F32),
                pltpu.VMEM((1, LANES), F32),
                dma((ITERS, 2)), dma((ITERS, 2)),
                dma((ITERS, 2, 3)), dma((ITERS, 2, 3)),
                dma((count,)), dma((count,)),
            ],
            compiler_params=pltpu.CompilerParams(collective_id=0, has_side_effects=True),
        )(right_side, reaction, weights)

    return jax.shard_map(
        local, mesh=mesh,
        in_specs=(P("gx", "gy"), P("gx", "gy"), P()),
        out_specs=(P("gx", "gy"), P("gx", "gy")),
        check_vma=False,
    )
```

```python
import functools

import jax
import jax.numpy as jnp
from jax import lax
from jax.experimental import pallas as pl
from jax.experimental.pallas import tpu as pltpu
from jax.sharding import PartitionSpec as P

ITERS = 4
SHIFT = 3.0
SMALL = 1e-06
LANES = 128
FOLD = 8
MESH = pl.DeviceIdType.MESH
F32 = jnp.float32
BF16 = jnp.bfloat16


def split(values):
    high = values.astype(BF16)
    return high, (values - high.astype(F32)).astype(BF16)


def lane_group(shape, width):
    return lax.broadcasted_iota(jnp.int32, shape, 1) // width


def pick(group, parts):
    chosen = parts[0]
    for index in range(1, len(parts)):
        chosen = jnp.where(group == index, parts[index], chosen)
    return chosen


def solve(gram):
    count = ITERS + 1
    initial = jnp.sqrt(gram[0][0] + SMALL)
    basis = [[1.0 / initial]]
    images = []
    applied = []
    upper = [[None] * ITERS for _ in range(count)]

    def times_gram(vector):
        out = []
        for row in range(count):
            total = vector[0] * gram[row][0]
            for col in range(1, len(vector)):
                total = total + vector[col] * gram[row][col]
            out.append(total)
        return out

    def inner(left, right):
        total = left[0] * right[0]
        for index in range(1, len(left)):
            total = total + left[index] * right[index]
        return total

    images.append(times_gram(basis[0]))
    for column in range(ITERS):
        prior = basis[column]
        candidate = [SHIFT * prior[0]]
        for index in range(1, len(prior)):
            candidate.append(SHIFT * prior[index] + prior[index - 1])
        candidate.append(prior[-1])
        applied.append(list(candidate))
        for earlier in range(column + 1):
            projected = inner(candidate, images[earlier])
            for index, value in enumerate(basis[earlier]):
                candidate[index] = candidate[index] - projected * value
            upper[earlier][column] = projected
        square = jnp.maximum(inner(candidate, times_gram(candidate)), 0.0)
        length = jnp.sqrt(square + SMALL)
        upper[column + 1][column] = length
        if column + 1 < ITERS:
            inverse = 1.0 / length
            basis.append([value * inverse for value in candidate])
            images.append(times_gram(basis[-1]))

    normal = [[None] * ITERS for _ in range(ITERS)]
    for row in range(ITERS):
        for col in range(row + 1):
            total = None
            for index in range(col + 2):
                term = upper[index][row] * upper[index][col]
                total = term if total is None else total + term
            normal[row][col] = total
    factor = [[None] * ITERS for _ in range(ITERS)]
    inverse = [None] * ITERS
    for col in range(ITERS):
        for row in range(col, ITERS):
            accum = normal[row][col]
            for index in range(col):
                accum = accum - factor[row][index] * factor[col][index]
            if row == col:
                factor[row][col] = jnp.sqrt(accum)
                inverse[col] = 1.0 / factor[row][col]
            else:
                factor[row][col] = accum * inverse[col]
    forward = []
    for row in range(ITERS):
        accum = initial * upper[0][row]
        for index in range(row):
            accum = accum - factor[row][index] * forward[index]
        forward.append(accum * inverse[row])
    coeffs = [None] * ITERS
    for row in reversed(range(ITERS)):
        accum = forward[row]
        for index in range(row + 1, ITERS):
            accum = accum - factor[index][row] * coeffs[index]
        coeffs[row] = accum * inverse[row]

    def combine(vectors, size):
        out = []
        for index in range(size):
            total = None
            for coeff, vector in zip(coeffs, vectors):
                if index < len(vector):
                    term = coeff * vector[index]
                    total = term if total is None else total + term
            out.append(total)
        return out

    return combine(basis, ITERS), combine(applied, count)


def kernel(
    nx, ny, b_ref, reac_ref, k_ref, x_ref, r_ref,
    kpad, whi, wlo, ybuf, wbuf, ebuf, hrow, hedge, gall, gown,
    row_send, row_recv, edge_send, edge_recv, g_send, g_recv,
):
    rows, cols = b_ref.shape
    width = k_ref.shape[0]
    rad = width // 2
    span = rows + 2 * rad
    tiles = cols // LANES
    subs = rows // 8
    count = nx * ny
    gx, gy = lax.axis_index("gx"), lax.axis_index("gy")
    me = gx * ny + gy

    hrow[...] = jnp.zeros_like(hrow)
    hedge[...] = jnp.zeros_like(hedge)

    barrier = pltpu.get_barrier_semaphore()

    def other(step):
        target = lax.rem(me + step, count)
        return (target // ny, lax.rem(target, ny))

    def greet(step, carry):
        pl.semaphore_signal(barrier, inc=1, device_id=other(step), device_id_type=MESH)
        return carry

    lax.fori_loop(1, count, greet, 0)

    exists_x = {-1: gx > 0, 0: None, 1: gx < nx - 1}
    exists_y = {-1: gy > 0, 1: gy < ny - 1}

    def both(dx, dy):
        if dx == 0:
            return exists_y[dy]
        if dy == 0:
            return exists_x[dx]
        return jnp.logical_and(exists_x[dx], exists_y[dy])

    def source(step):
        return b_ref if step == 0 else wbuf.at[step - 1]

    def row_copy(step, dx):
        slot = 0 if dx == 1 else 1
        return pltpu.make_async_remote_copy(
            src_ref=source(step), dst_ref=hrow.at[step, slot],
            send_sem=row_send.at[step, slot], recv_sem=row_recv.at[step, slot],
            device_id=(gx + dx, gy), device_id_type=MESH,
        )

    def edge_copy(step, dx, dy):
        side = 1 if dy == -1 else 0
        group = 1 - dx
        return pltpu.make_async_remote_copy(
            src_ref=ebuf.at[step, side], dst_ref=hedge.at[step, side, group],
            send_sem=edge_send.at[step, side, group], recv_sem=edge_recv.at[step, side, group],
            device_id=(gx + dx, gy + dy), device_id_type=MESH,
        )

    edges = [(dx, dy) for dx in (-1, 1, 0) for dy in (-1, 1)]

    def start_all(step):
        for dx in (-1, 1):
            pl.when(both(dx, 0))(lambda dx=dx: row_copy(step, dx).start())
        for dx, dy in edges:
            pl.when(both(dx, dy))(lambda dx=dx, dy=dy: edge_copy(step, dx, dy).start())

    def wait_recv_all(step):
        for dx in (-1, 1):
            pl.when(both(-dx, 0))(lambda dx=dx: row_copy(step, dx).wait_recv())
        for dx, dy in edges:
            pl.when(both(-dx, -dy))(lambda dx=dx, dy=dy: edge_copy(step, dx, dy).wait_recv())

    def wait_send_all(step):
        for dx in (-1, 1):
            pl.when(both(dx, 0))(lambda dx=dx: row_copy(step, dx).wait_send())
        for dx, dy in edges:
            pl.when(both(dx, dy))(lambda dx=dx, dy=dy: edge_copy(step, dx, dy).wait_send())

    group8 = lane_group((8, LANES), rad)

    def pack_edges(step, values):
        first = values[:, :LANES]
        last = values[:, cols - LANES:]
        lefts, rights = [], []
        for t in range(subs):
            piece = first[8 * t: 8 * t + 8]
            lefts.append(pltpu.roll(piece, (rad * t) % LANES, 1) if t else piece)
            piece = last[8 * t: 8 * t + 8]
            move = (rad * t - (LANES - rad)) % LANES
            rights.append(pltpu.roll(piece, move, 1) if move else piece)
        ebuf[step, 1] = pick(group8, lefts)
        ebuf[step, 0] = pick(group8, rights)

    pack_edges(0, b_ref[...])

    kpad[...] = jnp.zeros_like(kpad)
    kpad[:width, :width] = k_ref[...]
    kpad[...] = kpad[...].T
    group_span = lane_group((span, LANES), rows)
    per_tile = LANES // rows
    blocks = -(-width // (2 * FOLD))
    whole = FOLD * rows
    for q in range(blocks):
        for h in range(2):
            first = 2 * FOLD * q + FOLD * h
            base = (2 * q + h) * LANES
            for t in range(whole // LANES):
                parts = []
                for u in range(per_tile):
                    b = first + per_tile * t + u
                    if b < width:
                        line = jnp.broadcast_to(kpad[b: b + 1, :], (span, LANES))
                        move = (rows * u - 2 * rad) % LANES
                        parts.append(pltpu.roll(line, move, 1, stride=1, stride_axis=0))
                    else:
                        parts.append(jnp.zeros((span, LANES), F32))
                block = pick(group_span, parts)
                block = jnp.concatenate([block, jnp.zeros((LANES - span, LANES), F32)], axis=0)
                high, low = split(block)
                whi[base: base + LANES, t * LANES: (t + 1) * LANES] = high
                wlo[base: base + LANES, t * LANES: (t + 1) * LANES] = low

    pl.semaphore_wait(barrier, count - 1)
    start_all(0)

    steps_m = cols + 2 * FOLD
    group_cols = lane_group((cols, LANES), rows)
    offset = reac_ref[...] - SHIFT

    def fold8(values):
        total = values[:8]
        for t in range(1, subs):
            total = total + values[8 * t: 8 * t + 8]
        out = total[:, :LANES]
        for t in range(1, tiles):
            out = out + total[:, t * LANES: (t + 1) * LANES]
        return jnp.sum(out, axis=0, keepdims=True)

    def multiply(lhs_tiles, *accs):
        work = [(whi, q, lhs_tiles[q]) for q in range(blocks)] + [(wlo, q, lhs_tiles[q][:1]) for q in range(blocks)]
        lanes_of = [[], []]
        load = [0, 0]
        for item in work:
            unit = 0 if load[0] <= load[1] else 1
            lanes_of[unit].append(item)
            load[unit] += len(item[2])
        def push(unit, index):
            table, q, _ = lanes_of[unit][index]
            pltpu.matmul_push_rhs(
                table[q * 2 * LANES: (q + 1) * 2 * LANES, :], staging_register=index % 2, mxu_index=unit
            )
        for unit in range(2):
            push(unit, 0)
        for index in range(max(map(len, lanes_of))):
            for unit in range(2):
                if index + 1 < len(lanes_of[unit]):
                    push(unit, index + 1)
            for unit in range(2):
                if index < len(lanes_of[unit]):
                    for place, lhs in enumerate(lanes_of[unit][index][2]):
                        pltpu.matmul_acc_lhs(
                            accs[unit], lhs, load_staged_rhs=index % 2 if place == 0 else None
                        )
        parts = [pltpu.matmul_pop(accs[unit]) for unit in range(2)]
        ybuf[...] = parts[0] + parts[1]

    vectors = [b_ref[...]]
    products = {(0, 0): fold8(vectors[0] * vectors[0])}

    for step in range(ITERS):
        own = vectors[step]
        wait_recv_all(step)
        above, below = hrow[step, 0], hrow[step, 1]
        blank = jnp.zeros((LANES - span, LANES), F32)
        centre = []
        for t in range(tiles):
            part = slice(t * LANES, (t + 1) * LANES)
            tile = jnp.concatenate([above[:, part], own[:, part], below[:, part], blank], axis=0)
            centre.append(tile.T)
        sides = []
        for group in range(3):
            left = hedge[step, 0, group]
            right = hedge[step, 1, group] if True else None
            for t in range(subs):
                move = (-rad * t) % LANES
                from_left = pltpu.roll(left, move, 1) if move else left
                move = (rad - rad * t) % LANES
                from_right = pltpu.roll(right, move, 1) if move else right
                sides.append(jnp.where(group8 == 0, from_left, from_right))
        side = jnp.concatenate(sides + [blank], axis=0).T
        padded = jnp.concatenate([side[:rad]] + centre + [side[rad: 2 * rad]], axis=0)
        zero = jnp.zeros((FOLD, LANES), F32)
        plain = jnp.concatenate([zero] * 3 + [padded] + [zero], axis=0)
        moved = jnp.concatenate([zero] * 4 + [padded], axis=0)
        high, low = split(jnp.concatenate([plain, moved], axis=1))
        top = 2 * FOLD * blocks
        lhs_tiles = [
            (high[top - 2 * FOLD * q: top - 2 * FOLD * q + steps_m], low[top - 2 * FOLD * q: top - 2 * FOLD * q + steps_m])
            for q in range(blocks)
        ]
        pl.run_scoped(functools.partial(multiply, lhs_tiles), *[pltpu.ACC(unit)(ybuf.shape, F32) for unit in range(2)])
        parts = []
        for u in range(per_tile):
            total = None
            for t in range(whole // LANES):
                start = FOLD - per_tile * t - u
                piece = ybuf[start: start + cols, t * LANES: (t + 1) * LANES]
                total = piece if total is None else total + piece
            parts.append(total)
        chosen = pick(group_cols, parts)
        pieces = []
        for t in range(tiles):
            turned = chosen[t * LANES: (t + 1) * LANES].T
            total = turned[:rows]
            for u in range(1, per_tile):
                total = total + turned[rows * u: rows * (u + 1)]
            pieces.append(total)
        fresh = offset * own - jnp.concatenate(pieces, axis=1)
        wbuf[step] = fresh
        if step + 1 < ITERS:
            pack_edges(step + 1, fresh)
            start_all(step + 1)
        vectors.append(fresh)
        for earlier in range(step + 2):
            products[(earlier, step + 1)] = fold8(vectors[earlier] * fresh)

    order = sorted(products)
    stack = [products[pair] for pair in order]
    table = jnp.concatenate(stack + [jnp.zeros((LANES - len(stack), LANES), F32)], axis=0)
    line = jnp.sum(table.T, axis=0, keepdims=True)
    gown[...] = line
    gall[me] = line

    def gram_copy(step):
        return pltpu.make_async_remote_copy(
            src_ref=gown, dst_ref=gall.at[me],
            send_sem=g_send.at[step], recv_sem=g_recv.at[me],
            device_id=other(step), device_id_type=MESH,
        )

    def gram_arrival(step):
        sender = lax.rem(me + step, count)
        return pltpu.make_async_remote_copy(
            src_ref=gown, dst_ref=gall.at[sender],
            send_sem=g_send.at[step], recv_sem=g_recv.at[sender],
            device_id=other(step), device_id_type=MESH,
        )

    def send(step, carry):
        gram_copy(step).start()
        return carry

    def receive(step, carry):
        gram_arrival(step).wait_recv()
        return carry

    def sent(step, carry):
        gram_copy(step).wait_send()
        return carry

    lax.fori_loop(1, count, send, 0)
    for step in range(ITERS):
        wait_send_all(step)
    lax.fori_loop(1, count, receive, 0)
    total = jnp.sum(gall[...], axis=0)
    spread = jnp.broadcast_to(total, (LANES, LANES)).T
    gram = [[None] * (ITERS + 1) for _ in range(ITERS + 1)]
    for index, (i, j) in enumerate(order):
        gram[i][j] = gram[j][i] = spread[index: index + 1]
    at_solution, at_applied = solve(gram)
    wide = lambda value: jnp.concatenate([value] * tiles, axis=1)
    answer = wide(at_solution[0]) * vectors[0]
    for index in range(1, ITERS):
        answer = answer + wide(at_solution[index]) * vectors[index]
    x_ref[...] = answer
    image = wide(at_applied[0]) * vectors[0]
    for index in range(1, ITERS + 1):
        image = image + wide(at_applied[index]) * vectors[index]
    r_ref[...] = vectors[0] - image
    lax.fori_loop(1, count, sent, 0)


def solution(mesh):
    nx, ny = mesh.shape["gx"], mesh.shape["gy"]
    count = nx * ny

    def local(right_side, reaction, weights):
        rows, cols = right_side.shape
        width = weights.shape[0]
        blocks = -(-width // (2 * FOLD))
        depth = blocks * 2 * LANES
        block = jax.ShapeDtypeStruct((rows, cols), F32)
        in_vmem = pl.BlockSpec(memory_space=pltpu.VMEM)
        dma = pltpu.SemaphoreType.DMA
        return pl.pallas_call(
            functools.partial(kernel, nx, ny),
            name="gmres_cycle",
            out_shape=(block, block),
            in_specs=[in_vmem] * 3,
            out_specs=(in_vmem, in_vmem),
            scratch_shapes=[
                pltpu.VMEM((LANES, LANES), F32),
                pltpu.VMEM((depth, FOLD * rows), BF16),
                pltpu.VMEM((depth, FOLD * rows), BF16),
                pltpu.VMEM((cols + 2 * FOLD, FOLD * rows), F32),
                pltpu.VMEM((ITERS, rows, cols), F32),
                pltpu.VMEM((ITERS, 2, 8, LANES), F32),
                pltpu.VMEM((ITERS, 2, rows, cols), F32),
                pltpu.VMEM((ITERS, 2, 3, 8, LANES), F32),
                pltpu.VMEM((count, 1, LANES), F32),
                pltpu.VMEM((1, LANES), F32),
                dma((ITERS, 2)), dma((ITERS, 2)),
                dma((ITERS, 2, 3)), dma((ITERS, 2, 3)),
                dma((count,)), dma((count,)),
            ],
            compiler_params=pltpu.CompilerParams(collective_id=0, has_side_effects=True),
        )(right_side, reaction, weights)

    return jax.shard_map(
        local, mesh=mesh,
        in_specs=(P("gx", "gy"), P("gx", "gy"), P()),
        out_specs=(P("gx", "gy"), P("gx", "gy")),
        check_vma=False,
    )
```
